128 devices in a mesh: gx: 8 (over z, core), gy: 16 (over x, y).
Axes of the slice: x: 4, y: 4, z: 4, core: 2. Of those that a mesh axis runs over, the one named last changes fastest.
Arguments:
- vorticity: float32 [8192, 8192], P('gx', 'gy'), may hold values from -6 to 6
- tile_list: int32 [128, 64], P(('gx', 'gy')), may hold values from 0 to 4095, as said below
- float_slot: int32 [262144], P(('gx', 'gy')), may hold values from 0 to 63, as said below
- float_cell: int32 [2, 262144], P(None, ('gx', 'gy')), may hold values from 1 to 125
- float_frac: float32 [2, 262144], P(None, ('gx', 'gy')), may hold values from 0 to 1
Outputs:
- float_velocity: float32 [2, 262144], P(None, ('gx', 'gy'))
The draws below stay inside these ranges and needn't reach their ends.
Inputs may be any that keep to these rules, and one draw needn't show every extreme that they name: `tile_list`: row b lists the 64 tiles used by float block b; tile t covers the 128 x 128 cells from row (t // 64) * 128 and column (t % 64) * 128. The 64 tiles of a row lie in the blocks of vorticity held by 64 different devices, and one device's block is named by every row. `float_slot`: at most 64 floats of one block name the same position; in every block the position whose tile lies in the device block named by every row of tile_list is named by exactly 64 floats.
All inputs are finite; a program needn't handle non-finite values.
Results may differ from the reference program's by a relative error of at most 0.0031.
Values may be sent and summed in bfloat16 or wider, within the bound.
No kernel may reach another device: no remote copies, remote signals or barrier semaphores. Data moves between devices by JAX's collectives and lax.ppermute only.
A program may use at most 128 MiB of HBM per device.

```python
import math
import jax
import jax.numpy as jnp
from jax import lax

N = 8192
TILE = 128
F_DEV = 2048
DRIFTER_GROUPS = 128
K = 64
FCAP = 64
FLOATS = 262144
TR = 8
TC = 4
TILES_DEV = 32
NTC = 64


def float_plan(key):
    base = jax.random.fold_in(key, 7)
    key_hot, key_score, random_lean, key_order = jax.random.split(base, 4)
    busiest_block = jax.random.randint(key_hot, (), 0, DRIFTER_GROUPS)
    owning_positions = jnp.arange(DRIFTER_GROUPS, dtype=jnp.int32)
    group_score = jax.random.randint(key_score, (DRIFTER_GROUPS, DRIFTER_GROUPS), 0, 65536)
    affinity_reward = jax.random.randint(random_lean, (DRIFTER_GROUPS,), 0, 4)
    added_reward = jnp.where(owning_positions == busiest_block, 1048576, 0)
    overall_total = (group_score + affinity_reward[None, :] * 16384 + added_reward[None, :]) * DRIFTER_GROUPS + owning_positions[None, :]
    chosen = lax.top_k(overall_total, K)[1].astype(jnp.int32)
    order_score = jax.random.randint(key_order, (DRIFTER_GROUPS, K), 0, 65536) * K + jnp.arange(K, dtype=jnp.int32)[None, :]
    order = lax.top_k(order_score, K)[1]
    owners = jnp.take_along_axis(chosen, order, axis=1)
    hot_slot = jnp.sum(jnp.where(owners == busiest_block, jnp.arange(K, dtype=jnp.int32)[None, :], 0), axis=1)
    return (owners, hot_slot)


def draw_tile_list(key, part):
    owners, hot_slot = float_plan(key)
    local_tile = jax.random.randint(jax.random.fold_in(key, 9), (DRIFTER_GROUPS, K), 0, TILES_DEV)
    group_cols = NTC // TC
    grid_row = owners // group_cols * TR + local_tile // TC
    grid_col = owners % group_cols * TC + local_tile % TC
    return (grid_row * NTC + grid_col).astype(jnp.int32)


def draw_float_slot(key, part):
    owners, hot_slot = float_plan(key)
    key_weight, key_order = jax.random.split(jax.random.fold_in(key, 13))
    weights = jax.random.randint(key_weight, (DRIFTER_GROUPS, K - 1), 2, 4)
    remainder = F_DEV - FCAP
    bounds = jnp.cumsum(weights * remainder, axis=1) // jnp.sum(weights, axis=1, keepdims=True)
    order_score = jax.random.randint(key_order, (DRIFTER_GROUPS, F_DEV), 0, 65536) * F_DEV + jnp.arange(F_DEV, dtype=jnp.int32)[None, :]
    order = lax.top_k(order_score, F_DEV)[1]
    turn = jnp.arange(F_DEV, dtype=jnp.int32)
    other = jnp.sum((bounds[:, None, :] <= (turn - FCAP)[None, :, None]).astype(jnp.int32), axis=2)
    other = other + (other >= hot_slot[:, None]).astype(jnp.int32)
    by_turn = jnp.where(turn[None, :] < FCAP, hot_slot[:, None], other)
    block_ids = jnp.broadcast_to(jnp.arange(DRIFTER_GROUPS, dtype=jnp.int32)[:, None], (DRIFTER_GROUPS, F_DEV))
    slots = jnp.zeros((DRIFTER_GROUPS, F_DEV), jnp.int32).at[block_ids, order].set(by_turn)
    return slots.reshape(DRIFTER_GROUPS * F_DEV).astype(jnp.int32)


def draw_vorticity(key, part):
    noise_key = jax.random.fold_in(key, 3)
    return jnp.clip(jax.random.normal(noise_key, (N, N), jnp.float32), -6.0, 6.0)


def with_ends(array, own_key, low, largest):
    shape = array.shape
    place = [jax.random.randint(jax.random.fold_in(own_key, axis), (), 0, shape[axis]) for axis in range(len(shape))]
    array = array.at[tuple(place)].set(low)
    longest = shape.index(max(shape))
    place[longest] = (place[longest] + 1) % shape[longest]
    return array.at[tuple(place)].set(largest)


def levels(stream_key, extent, pieces, low, largest):
    gain, own = 1.0, jax.random.fold_in(stream_key, 6)
    for dim, parts in pieces:
        steps = jnp.exp(jax.random.uniform(jax.random.fold_in(own, dim), (parts,), jnp.float32, low / len(pieces), largest / len(pieces)))
        gain = gain * jnp.repeat(steps, extent[dim] // parts).reshape([-1 if axis == dim else 1 for axis in range(len(extent))])
    return gain


def setup_inputs(seed: int = 0) -> dict:
    splits = jax.random.split(jax.random.key(seed), 6)
    return {
        "vorticity": draw_vorticity(jax.random.fold_in(splits[5], 71), 0),
        "tile_list": draw_tile_list(jax.random.fold_in(splits[5], 71), 0),
        "float_slot": draw_float_slot(jax.random.fold_in(splits[5], 71), 0),
        "float_cell": with_ends(jax.random.randint(splits[3], (2, FLOATS), 1, TILE - 2), jax.random.fold_in(splits[3], 1), 1, (TILE - 2) - 1).astype(jnp.int32),
        "float_frac": jnp.clip(1.0 * jax.random.uniform(splits[4], (2, FLOATS), jnp.float32) ** levels(splits[4], (2, FLOATS), ((1, 128),), -0.2, 0.2), 0.0, 1.0),
    }


def wavenumbers(index, length):
    signed = jnp.where(index < length // 2, index, index - length).astype(jnp.float32)
    wave = (2.0 * math.pi / length) * signed
    slope = jnp.where(index == length // 2, 0.0, wave)
    return wave, slope, (2.0 + jnp.cos(wave)) / 3.0


def spline_weights(position):
    complement = 1.0 - position
    cubed = position * position * position
    return (complement * complement * complement / 6.0,
            (3.0 * cubed - 6.0 * position * position + 4.0) / 6.0,
            (-3.0 * cubed + 3.0 * position * position + 3.0 * position + 1.0) / 6.0,
            cubed / 6.0)


def reference(vorticity, tile_list, float_slot, float_cell, float_frac):
    length = vorticity.shape[0]
    spectrum = jnp.fft.rfft2(vorticity)
    row_wave, row_slope, row_prefilter = wavenumbers(jnp.arange(length, dtype=jnp.int32), length)
    col_wave, col_slope, col_prefilter = wavenumbers(jnp.arange(length // 2 + 1, dtype=jnp.int32), length)
    kappa = math.pi / length
    factor = 1.0 / ((row_wave[:, None] * row_wave[:, None] + col_wave[None, :] * col_wave[None, :] + kappa * kappa)
                    * (row_prefilter[:, None] * col_prefilter[None, :]))
    spec_u = 1j * (row_slope[:, None] * factor) * spectrum
    spec_v = -1j * (col_slope[None, :] * factor) * spectrum
    coeff_u = jnp.fft.irfft2(spec_u, s=(length, length)).astype(jnp.float32)
    coeff_v = jnp.fft.irfft2(spec_v, s=(length, length)).astype(jnp.float32)
    coeffs = lax.optimization_barrier(jnp.stack([coeff_u, coeff_v]).astype(jnp.bfloat16))
    per_row = length // TILE
    float_count = float_slot.shape[0]
    block_len = float_count // tile_list.shape[0]
    owner_block = jnp.arange(float_count, dtype=jnp.int32) // block_len
    tile_number = tile_list[owner_block, float_slot]
    row_start = (tile_number // per_row) * TILE + float_cell[0] - 1
    col_start = (tile_number % per_row) * TILE + float_cell[1] - 1
    offsets = jnp.arange(4, dtype=jnp.int32)
    row_cells = row_start[:, None] + offsets[None, :]
    col_cells = col_start[:, None] + offsets[None, :]
    window = coeffs[:, row_cells[:, :, None], col_cells[:, None, :]]
    down = lax.optimization_barrier(jnp.stack(spline_weights(float_frac[0]), axis=1).astype(jnp.bfloat16))
    across = jnp.stack(spline_weights(float_frac[1]), axis=1)
    inner = jnp.einsum("fi,cfij->cfj", down.astype(jnp.float32), window.astype(jnp.float32))
    return jnp.einsum("fj,cfj->cf", across, inner)
```

```python
import functools
import math

import jax
import jax.numpy as jnp
import numpy as np
from jax import lax
from jax.experimental import pallas as pl
from jax.experimental.pallas import tpu as pltpu
from jax.sharding import PartitionSpec as P

N = 8192
KAPPA = math.pi / N
BF = jnp.bfloat16
F32 = jnp.float32
VMEM = 60 * 1024 * 1024


def _mul_const(v, c, s):
    re, im = v
    if abs(s) < 1e-12:
        if abs(c - 1.0) < 1e-12:
            return v
        if abs(c + 1.0) < 1e-12:
            return _sub((None, None), v)
    if abs(c) < 1e-12:
        return _times_i(v, s)
    if re is None:
        return (im * -s, im * c)
    if im is None:
        return (re * c, re * s)
    if abs(abs(c) - abs(s)) < 1e-12:
        q = abs(c)
        a, b = (1 if c > 0 else -1), (1 if s > 0 else -1)
        if a == b:
            return ((re - im) * (q * a), (re + im) * (q * a))
        return ((re + im) * (q * a), (im - re) * (q * a))
    return (re * c - im * s, re * s + im * c)


def _add(x, y):
    def one(p, q):
        if p is None:
            return q
        return p if q is None else p + q

    return (one(x[0], y[0]), one(x[1], y[1]))


def _sub(x, y):
    def one(p, q):
        if q is None:
            return p
        return -q if p is None else p - q

    return (one(x[0], y[0]), one(x[1], y[1]))


def _times_i(v, sign):
    re, im = v
    if sign > 0:
        return (None if im is None else -im, re)
    return (im, None if re is None else -re)


def fft_list(xs, sign):
    n = len(xs)
    if n == 1:
        return xs
    if n == 2:
        return [_add(xs[0], xs[1]), _sub(xs[0], xs[1])]
    if n == 4:
        s, d = _add(xs[0], xs[2]), _sub(xs[0], xs[2])
        t, e = _add(xs[1], xs[3]), _times_i(_sub(xs[1], xs[3]), sign)
        return [_add(s, t), _add(d, e), _sub(s, t), _sub(d, e)]
    outer = 4 if n % 4 == 0 and n > 8 else 2
    inner = n // outer
    cols = [fft_list(xs[j::outer], sign) for j in range(outer)]
    out = [None] * n
    for k0 in range(inner):
        row = []
        for j in range(outer):
            ang = sign * 2.0 * math.pi * j * k0 / n
            row.append(_mul_const(cols[j][k0], math.cos(ang), math.sin(ang)))
        for k1, v in enumerate(fft_list(row, sign)):
            out[k0 + inner * k1] = v
    return out


def split2(x):
    hi = x.astype(BF)
    return hi, (x - hi.astype(F32)).astype(BF)


def table_split(t):
    t = np.asarray(t, np.float64)
    hi = t.astype(np.float32).astype(jnp.bfloat16)
    lo = (t - hi.astype(np.float64)).astype(np.float32).astype(jnp.bfloat16)
    return hi, lo


def mm(a, b):
    return lax.dot_general(a, b, (((1,), (0,)), ((), ())), preferred_element_type=F32)


def mm_nt(a, b):
    return lax.dot_general(a, b, (((1,), (1,)), ((), ())), preferred_element_type=F32)


def mm_tn(a, b):
    return lax.dot_general(a, b, (((0,), (0,)), ((), ())), preferred_element_type=F32)


def call(kernel, out_shape, scratch, *args, specs=None):
    params = dict(
        out_shape=out_shape,
        scratch_shapes=scratch,
        compiler_params=pltpu.CompilerParams(vmem_limit_bytes=VMEM),
    )
    if specs is not None:
        params["in_specs"] = specs
    return pl.pallas_call(kernel, **params)(*args)


def cast_kernel(x_ref, o_ref):
    s = lax.broadcasted_iota(jnp.int32, (8, 8, 128), 1)

    def handed(x, rows, shift):
        error = jnp.where(rows, x.astype(BF).astype(F32) - x, 0.0)
        return x - pltpu.roll(error, shift, 1)

    for q in range(4):
        x = x_ref[:, q * 128 : (q + 1) * 128].reshape(8, 8, 128)
        x = handed(x, s % 2 == 0, 1)
        x = handed(x, s % 4 == 1, 2)
        o_ref[0, q] = x.reshape(64, 128).astype(BF)


def cast_block(vorticity):
    return pl.pallas_call(
        cast_kernel,
        grid=(16,),
        in_specs=[pl.BlockSpec((64, 512), lambda i: (i, 0))],
        out_specs=pl.BlockSpec((1, 4, 64, 128), lambda i: (i, 0, 0, 0)),
        out_shape=jax.ShapeDtypeStruct((16, 4, 64, 128), BF),
    )(vorticity)


def rows_kernel(x_ref, twr_ref, twi_ref, thi_ref, tlo_ref, alt_ref, o_ref, a_ref, yhi_ref, ylo_ref):
    def first(t, carry):
        rows = pl.ds(pl.multiple_of(t * 16, 16), 16)
        for j in range(8):
            xs = [(x_ref[8 * i + j, rows, :].astype(F32), None) for i in range(8)]
            ys = fft_list(xs, -1.0)
            for k0 in range(5):
                ang = -2.0 * math.pi * j * k0 / 64
                re, im = _mul_const(ys[k0], math.cos(ang), math.sin(ang))
                zero = jnp.zeros((16, 128), F32)
                a_ref[k0, j, 0, rows, :] = zero if re is None else re
                a_ref[k0, j, 1, rows, :] = zero if im is None else im
        return carry

    lax.fori_loop(0, 4, first, 0)

    def put(k, re, im, rows):
        cr, ci = twr_ref[k], twi_ref[k]
        yr, yi = re * cr - im * ci, re * ci + im * cr
        hr, lr = split2(yr)
        hi, li = split2(yi)
        yhi_ref[k, rows, 0:128] = hr
        yhi_ref[k, rows, 128:256] = hi
        ylo_ref[k, rows, 0:128] = lr
        ylo_ref[k, rows, 128:256] = li

    def second(t, carry):
        rows = pl.ds(pl.multiple_of(t * 16, 16), 16)
        for k0 in range(5):
            zs = fft_list([(a_ref[k0, j, 0, rows, :], a_ref[k0, j, 1, rows, :]) for j in range(8)], -1.0)
            for k1 in range(8):
                k = k0 + 8 * k1
                re, im = zs[k1]
                put(k, re, im, rows)
                if k0 in (1, 2, 3):
                    put(64 - k, re, -im, rows)
        return carry

    lax.fori_loop(0, 4, second, 0)

    def third(kap, carry):
        yhi = yhi_ref[pl.ds(2 * kap, 2)].reshape(128, 256)
        ylo = ylo_ref[pl.ds(2 * kap, 2)].reshape(128, 256)
        z = mm_nt(thi_ref[...], yhi) + mm_nt(tlo_ref[...], yhi) + mm_nt(thi_ref[...], ylo)
        zb = z.astype(BF)
        for g in range(4):
            for c in range(2):
                o_ref[4 * kap + g, c] = zb[c * 64 + 16 * g : c * 64 + 16 * g + 16, :]
        return carry

    lax.fori_loop(0, 32, third, 0)

    nyq = mm_nt(alt_ref[...], yhi_ref[0:2].reshape(128, 256)) + mm_nt(
        alt_ref[...], ylo_ref[0:2].reshape(128, 256)
    )
    lane = lax.broadcasted_iota(jnp.int32, (16, 128), 1)
    sub = lax.broadcasted_iota(jnp.int32, (16, 128), 0)
    old = o_ref[0, 1].astype(F32)
    o_ref[0, 1] = jnp.where((lane < 64) & (sub == 0), nyq, old).astype(BF)


@functools.cache
def rows_tables():
    k = np.arange(64)[:, None, None]
    b = np.arange(128)[None, None, :]
    tw = np.exp(-2j * np.pi * k * b / N)
    w = np.exp(-2j * np.pi * np.arange(64)[:, None] * np.arange(128)[None, :] / 128)
    t = np.block([[w.real, -w.imag], [w.imag, w.real]])
    alt = np.zeros((16, 256))
    alt[0, :128] = (-1.0) ** np.arange(128)
    hi, lo = table_split(t)
    return (
        tw.real.astype(np.float32),
        tw.imag.astype(np.float32),
        hi,
        lo,
        alt.astype(np.float32).astype(jnp.bfloat16),
    )


def rows_forward(x):
    return call(
        rows_kernel,
        jax.ShapeDtypeStruct((128, 2, 16, 128), BF),
        [
            pltpu.VMEM((5, 8, 2, 64, 128), F32),
            pltpu.VMEM((64, 64, 256), BF),
            pltpu.VMEM((64, 64, 256), BF),
        ],
        x,
        *rows_tables(),
    )


def fft128(load, store, a_ref, rows, sign):
    for j in range(8):
        ys = fft_list([load(8 * i + j) for i in range(16)], sign)
        for k0 in range(16):
            ang = sign * 2.0 * math.pi * j * k0 / 128
            re, im = _mul_const(ys[k0], math.cos(ang), math.sin(ang))
            a_ref[k0, j, 0, rows, :] = re
            a_ref[k0, j, 1, rows, :] = im
    for k0 in range(16):
        zs = fft_list([(a_ref[k0, j, 0, rows, :], a_ref[k0, j, 1, rows, :]) for j in range(8)], sign)
        for k1 in range(8):
            store(k0 + 16 * k1, zs[k1])


def cols_kernel(
    x_ref, twr_ref, twi_ref, tw2r_ref, tw2i_ref, fhi_ref, flo_ref, bhi_ref, blo_ref,
    wm2_ref, pm_ref, sm_ref, del_ref, wn2_ref, pn_ref, sn_ref, hm_ref,
    o_ref,
    x32_ref, a_ref, yhi_ref, ylo_ref, e_ref, ce_ref, z_ref, shi_ref, slo_ref, p_ref,
):
    def widen(t, carry):
        for u in range(8):
            x32_ref[8 * t + u] = x_ref[8 * t + u].astype(F32)
        return carry

    lax.fori_loop(0, 16, widen, 0)

    def forward(hh, carry):
        rows = pl.ds(pl.multiple_of(hh * 8, 8), 8)

        def store(k, v):
            re, im = v
            cr, ci = twr_ref[k], twi_ref[k]
            yr, yi = re * cr - im * ci, re * ci + im * cr
            x32_ref[k, 0, rows, :] = yr
            x32_ref[k, 1, rows, :] = yi

            @pl.when(hh == 0)
            def _():
                back = (128 - k) % 128
                e_ref[0, back : back + 1, :] = re[0:1, :]
                e_ref[1, back : back + 1, :] = -im[0:1, :]

        fft128(lambda d: (x32_ref[d, 0, rows, :], x32_ref[d, 1, rows, :]), store, a_ref, rows, -1.0)
        return carry

    lax.fori_loop(0, 2, forward, 0)

    def second_split(t, carry):
        for u in range(8):
            k = 8 * t + u
            rows = pl.ds(pl.multiple_of(k * 16, 16), 16)
            hr, lr = split2(x32_ref[k, 0])
            hi, li = split2(x32_ref[k, 1])
            yhi_ref[rows, 0:128] = hr
            yhi_ref[rows, 128:256] = hi
            ylo_ref[rows, 0:128] = lr
            ylo_ref[rows, 128:256] = li
        return carry

    lax.fori_loop(0, 16, second_split, 0)

    fhi, flo = fhi_ref[...], flo_ref[...]

    er, ei = e_ref[0], e_ref[1]
    cr, ci = tw2r_ref[...], tw2i_ref[...]
    e_r, e_i = er * cr - ei * ci, er * ci + ei * cr
    hr, lr = split2(e_r)
    hi, li = split2(e_i)
    ehi = jnp.concatenate([hr, hi], axis=1)
    elo = jnp.concatenate([lr, li], axis=1)
    ce = mm(ehi, fhi) + mm(elo, fhi) + mm(ehi, flo)
    ce_ref[0] = ce[:, 0:128]
    ce_ref[1] = ce[:, 128:256]

    def matmul_f(t, carry):
        rows = pl.ds(pl.multiple_of(t * 256, 256), 256)
        z_ref[rows, :] = mm(yhi_ref[rows, :], fhi) + mm(ylo_ref[rows, :], fhi) + mm(yhi_ref[rows, :], flo)
        return carry

    lax.fori_loop(0, 8, matmul_f, 0)

    wn2, pn, sn, hm = wn2_ref[...], pn_ref[...], sn_ref[...], hm_ref[...]

    def spectral(t, carry):
        for u in range(8):
            k = 8 * t + u
            rows = pl.ds(pl.multiple_of(k * 16, 16), 16)
            zr, zi = z_ref[rows, 0:128], z_ref[rows, 128:256]
            fac = 1.0 / ((wm2_ref[k] + wn2 + KAPPA * KAPPA) * (pm_ref[k] * pn))
            dd = del_ref[k] * hm
            fr = fac * zr + dd * (ce_ref[0, pl.ds(k, 1), :] - zr)
            fi = fac * zi + dd * (ce_ref[1, pl.ds(k, 1), :] - zi)
            sm = sm_ref[k]
            for f, (re, im) in enumerate(((-sm * fi, sm * fr), (sn * fi, -sn * fr))):
                hr, lr = split2(re)
                hi, li = split2(im)
                shi_ref[f, rows, 0:128] = hr
                shi_ref[f, rows, 128:256] = hi
                slo_ref[f, rows, 0:128] = lr
                slo_ref[f, rows, 128:256] = li
        return carry

    lax.fori_loop(0, 16, spectral, 0)

    bhi, blo = bhi_ref[...], blo_ref[...]

    for f in range(2):

        def matmul_b(t, carry):
            rows = pl.ds(pl.multiple_of(t * 256, 256), 256)
            hi, lo = shi_ref[f, rows, :], slo_ref[f, rows, :]
            p_ref[rows, :] = mm(hi, bhi) + mm(lo, bhi) + mm(hi, blo)
            return carry

        lax.fori_loop(0, 8, matmul_b, 0)

        def inverse(hh, carry):
            rows = pl.ds(pl.multiple_of(hh * 8, 8), 8)

            def load(k):
                at = pl.ds(pl.multiple_of(k * 16 + hh * 8, 8), 8)
                re, im = p_ref[at, 0:128], p_ref[at, 128:256]
                cr, ci = twr_ref[k], twi_ref[k]
                return (re * cr + im * ci, im * cr - re * ci)

            def store(k, v):
                x32_ref[k, 0, rows, :] = v[0]
                x32_ref[k, 1, rows, :] = v[1]

            fft128(load, store, a_ref, rows, 1.0)
            return carry

        lax.fori_loop(0, 2, inverse, 0)

        def narrow(t, carry):
            for u in range(8):
                o_ref[8 * t + u, f] = x32_ref[8 * t + u].astype(BF)
            return carry

        lax.fori_loop(0, 16, narrow, 0)


def _wave(j, length):
    signed = np.where(j < length // 2, j, j - length).astype(np.float64)
    return 2.0 * np.pi / length * signed


@functools.cache
def cols_tables():
    lane = np.arange(128)
    kk = np.arange(128)[:, None]
    tw = np.exp(-2j * np.pi * kk * (lane % 64)[None, :] / N)
    w = np.exp(-2j * np.pi * np.outer(np.arange(64), np.arange(64)) / 64)
    eye = np.eye(2)
    wr, wi = np.kron(eye, w.real), np.kron(eye, w.imag)
    forward = np.block([[wr, wi], [-wi, wr]])
    backward = np.block([[wr, -wi], [wi, wr]])
    m = kk + 128 * (lane % 64)[None, :]
    wm = _wave(m, N)
    sm = np.where(m == N // 2, 0.0, wm)
    pm = (2.0 + np.cos(wm)) / 3.0
    f0 = 1.0 / ((wm**2 + KAPPA**2) * pm * float(N) ** 2)
    f1 = 1.0 / ((wm**2 + math.pi**2 + KAPPA**2) * pm * (1.0 / 3.0) * float(N) ** 2)
    delta = (f0 - f1) / 2.0

    def three(t):
        return np.asarray(t, np.float32)[:, None, :]

    twr, twi = tw.real.astype(np.float32), tw.imag.astype(np.float32)
    return (
        (three(twr), three(twi), twr, twi, *table_split(forward), *table_split(backward)),
        (three(wm**2), three(pm), three(sm), three(delta)),
    )


def cols_step(x, device):
    first, second = cols_tables()
    h = lax.broadcasted_iota(jnp.int32, (16, 128), 0)
    p = lax.broadcasted_iota(jnp.int32, (16, 128), 1) // 64
    n = 2 * (device // 4) + p + 64 * (16 * (device % 4) + h)
    wn = (2.0 * math.pi / N) * n.astype(F32)
    pn = (2.0 + jnp.cos(wn)) / 3.0 * (float(N) ** 2)
    pn = jnp.where(n == 0, pn, pn * 0.5)
    hm = jnp.where(n == 0, 1.0, 0.0).astype(F32)
    return call(
        cols_kernel,
        jax.ShapeDtypeStruct((128, 2, 2, 16, 128), BF),
        [
            pltpu.VMEM((128, 2, 16, 128), F32),
            pltpu.VMEM((16, 8, 2, 16, 128), F32),
            pltpu.VMEM((2048, 256), BF),
            pltpu.VMEM((2048, 256), BF),
            pltpu.VMEM((2, 128, 128), F32),
            pltpu.VMEM((2, 128, 128), F32),
            pltpu.VMEM((2048, 256), F32),
            pltpu.VMEM((2, 2048, 256), BF),
            pltpu.VMEM((2, 2048, 256), BF),
            pltpu.VMEM((2048, 256), F32),
        ],
        x, *first, *second, wn * wn, pn, wn, hm,
    )


def back_kernel(x_ref, t_ref, t0r_ref, t0i_ref, omr_ref, omi_ref, alt_ref, o_ref, s_ref, f_ref):
    table = t_ref[...]

    def first(kap, carry):
        cols = []
        for f in range(2):
            re = x_ref[pl.ds(4 * kap, 4), f, 0].reshape(64, 128)
            im = x_ref[pl.ds(4 * kap, 4), f, 1].reshape(64, 128)
            cols.append(jnp.concatenate([re, im, re, im], axis=0))
        s_ref[kap] = mm(table, jnp.concatenate(cols, axis=1))
        return carry

    lax.fori_loop(0, 32, first, 0)

    row = x_ref[0, 0, 1].astype(F32)[0:1, :]
    lane = lax.broadcasted_iota(jnp.int32, (128, 128), 1)
    s_ref[0, 0:128, 0:128] += jnp.where(lane < 64, alt_ref[...] * row, 0.0)

    low = lax.broadcasted_iota(jnp.int32, (8, 128), 1) < 64

    def second(t, carry):
        at = pl.ds(pl.multiple_of(t * 8, 8), 8)
        ati = pl.ds(pl.multiple_of(128 + t * 8, 8), 8)
        omr, omi = omr_ref[at, :], omi_ref[at, :]
        for f in range(2):
            tr, ti = t0r_ref[at, :], t0i_ref[at, :]
            xs = []
            for kap in range(32):
                re = s_ref[kap, at, f * 128 : (f + 1) * 128]
                im = s_ref[kap, ati, f * 128 : (f + 1) * 128]
                xs.append((re * tr - im * ti, re * ti + im * tr))
                tr, ti = tr * omr - ti * omi, tr * omi + ti * omr
            ys = fft_list(xs, 1.0)
            ts = []
            for x1 in range(32):
                re, im = ys[x1]
                ang = 2.0 * math.pi * x1 / 64
                ts.append(jnp.where(low, re, re * math.cos(ang) - im * math.sin(ang)))
            for e in range(16):
                ta, tb = ts[2 * e], ts[2 * e + 1]
                even = jnp.where(low, ta, pltpu.roll(tb, 64, 1))
                odd = jnp.where(low, pltpu.roll(ta, 64, 1), tb)
                f_ref[e // 2, f, e % 2, at, :] = even + odd
                f_ref[e // 2 + 8, f, e % 2, at, :] = even - odd
        return carry

    lax.fori_loop(0, 16, second, 0)

    def narrow(j, carry):
        o_ref[j] = f_ref[j].astype(BF)
        return carry

    lax.fori_loop(0, 16, narrow, 0)


@functools.cache
def back_tables():
    x0 = np.arange(128)
    e = np.exp(2j * np.pi * np.outer(x0, np.arange(64)) / 128)
    t = np.block([[e.real, -e.imag], [e.imag, e.real]])
    hi, lo = table_split(t)
    p = np.arange(128)[None, :] // 64
    t0 = np.exp(2j * np.pi * p * x0[:, None] / N)
    om = np.exp(2j * np.pi * 2 * x0[:, None] / N) * np.ones((1, 128))
    alt = ((-1.0) ** x0)[:, None] * np.ones((1, 128))
    f = lambda v: np.ascontiguousarray(v, np.float32)
    return (np.concatenate([hi, lo], axis=1), f(t0.real), f(t0.imag), f(om.real), f(om.imag), f(alt))


def rows_back(x):
    return call(
        back_kernel,
        jax.ShapeDtypeStruct((16, 2, 2, 128, 128), BF),
        [pltpu.VMEM((32, 256, 256), F32), pltpu.VMEM((16, 2, 2, 128, 128), F32)],
        x,
        *back_tables(),
    )


def split3(x):
    hi = x.astype(BF)
    rest = x - hi.astype(F32)
    mid = rest.astype(BF)
    return hi, mid, (rest - mid.astype(F32)).astype(BF)


def plan_kernel(list_ref, slot_ref, cell_ref, frac_ref, tri_ref, msg_ref, own_ref, s_ref, r_ref):
    slot = slot_ref[...]
    pick = lax.broadcasted_iota(jnp.int32, (64, 2048), 0) == slot
    tile = jnp.sum(jnp.where(pick, list_ref[...], 0), axis=0, keepdims=True)
    grid_row, grid_col = tile // 64, tile % 64
    owner = (grid_row // 8) * 16 + grid_col // 4
    local = ((grid_row % 8) * 4 + grid_col % 4).astype(F32)
    member = lax.broadcasted_iota(jnp.int32, (128, 2048), 0) == owner
    s_ref[...] = jnp.where(member, 1.0, 0.0).astype(BF)
    running = jnp.zeros((128, 1), F32)
    tri = tri_ref[...]
    for c in range(8):
        at = slice(c * 256, (c + 1) * 256)
        part = s_ref[:, at]
        total = mm(part, tri) + running
        rank = jnp.sum(part.astype(F32) * total, axis=0, keepdims=True) - 1.0
        running = total[:, 255:256]
        own_ref[1:2, at] = rank.astype(jnp.int32)
    own_ref[0:1, :] = owner
    rank = own_ref[1:2, :]
    place = lax.broadcasted_iota(jnp.int32, (64, 2048), 0) == rank
    r_ref[...] = jnp.where(place, 1.0, 0.0).astype(BF)

    def grouped(value):
        return mm_nt(s_ref[...] * value, r_ref[...])

    def exact(value):
        return sum(grouped(v) for v in split3(value))

    cells = [grouped(cell_ref[c : c + 1, :].astype(F32).astype(BF)) for c in range(2)]
    fracs = [exact(frac_ref[c : c + 1, :]) for c in range(2)]
    tiles = grouped(local.astype(BF))
    msg_ref[:, 0:128] = jnp.concatenate(cells, axis=1)
    msg_ref[:, 128:256] = jnp.concatenate(fracs, axis=1)
    msg_ref[:, 256:384] = jnp.concatenate([tiles, tiles], axis=1)


def plan_floats(tile_list, float_slot, float_cell, float_frac):
    tri = np.triu(np.ones((256, 256), np.float32)).astype(jnp.bfloat16)
    return call(
        plan_kernel,
        (
            jax.ShapeDtypeStruct((128, 384), F32),
            jax.ShapeDtypeStruct((2, 2048), jnp.int32),
        ),
        [pltpu.VMEM((128, 2048), BF), pltpu.VMEM((64, 2048), BF)],
        tile_list.reshape(64, 1),
        float_slot.reshape(1, 2048),
        float_cell,
        float_frac,
        tri,
    )


def weights_of(t):
    s = 1.0 - t
    cubed = t * t * t
    return (
        s * s * s / 6.0,
        (3.0 * cubed - 6.0 * t * t + 4.0) / 6.0,
        (-3.0 * cubed + 3.0 * t * t + 3.0 * t + 1.0) / 6.0,
        cubed / 6.0,
    )


def chain(e, ws):
    zero = jnp.zeros_like(ws[0])
    out = jnp.where(e == 3.0, ws[3], zero)
    for i in (2, 1, 0):
        out = jnp.where(e == float(i), ws[i], out)
    return out


def interp_kernel(tile_ref, c_ref, msg_ref, o_ref, w_ref, r_ref):
    low = lax.broadcasted_iota(jnp.int32, (64, 128), 1) < 64

    def paired(first):
        a, b = msg_ref[0:64, first : first + 128], msg_ref[64:128, first : first + 128]
        return jnp.where(low, a, pltpu.roll(b, 64, 1)), jnp.where(low, pltpu.roll(a, 64, 1), b)

    cell0, cell1 = paired(0)
    frac0, frac1 = paired(128)
    w_ref[0] = cell0 - 1.0
    w_ref[1] = cell1 - 1.0
    for i, w in enumerate(weights_of(frac0)):
        w_ref[2 + i] = w.astype(BF).astype(F32)
    for i, w in enumerate(weights_of(frac1)):
        w_ref[6 + i] = w

    iota64 = lax.broadcasted_iota(jnp.int32, (64, 128), 0).astype(F32)
    iota128 = lax.broadcasted_iota(jnp.int32, (128, 128), 0).astype(F32)
    lowrow = lax.broadcasted_iota(jnp.int32, (1, 128), 1) < 64
    low128 = lax.broadcasted_iota(jnp.int32, (128, 128), 1) < 64

    def step(i, carry):
        ta, tb = tile_ref[i], tile_ref[i + 64]
        par = jnp.where(lowrow, (ta % 2).astype(F32), (tb % 2).astype(F32))
        rows = [w_ref[v, pl.ds(i, 1), :] for v in range(10)]
        blocks = []
        for half in range(2):
            for xp in range(2):
                base = rows[0] - 64.0 * half + 1000.0 * jnp.abs(par - xp)
                blocks.append(chain(iota64 - base, [jnp.broadcast_to(w, (64, 128)) for w in rows[2:6]]))
        down = jnp.concatenate(blocks, axis=0).astype(BF)
        across = chain(iota128 - rows[1], [jnp.broadcast_to(w, (128, 128)) for w in rows[6:10]])
        for f in range(2):
            inner = []
            for tile in (ta, tb):
                tr, xh = tile // 4, (tile % 4) // 2
                lhs = jnp.concatenate([c_ref[2 * tr, f, xh], c_ref[2 * tr + 1, f, xh]], axis=1)
                inner.append(mm(lhs, down))
            both = jnp.where(low128, inner[0], inner[1])
            r_ref[f, pl.ds(i, 1), :] = jnp.sum(both * across, axis=0, keepdims=True)
        return carry

    lax.fori_loop(0, 64, step, 0)
    u, v = r_ref[0], r_ref[1]
    o_ref[0:64, :] = jnp.where(low, u, pltpu.roll(v, 64, 1))
    o_ref[64:128, :] = jnp.where(low, pltpu.roll(u, 64, 1), v)


def interpolate(tiles, coeffs, message):
    return call(
        interp_kernel,
        jax.ShapeDtypeStruct((128, 128), F32),
        [pltpu.VMEM((10, 64, 128), F32), pltpu.VMEM((2, 64, 128), F32)],
        tiles,
        coeffs,
        message,
        specs=[
            pl.BlockSpec(memory_space=pltpu.SMEM),
            pl.BlockSpec(memory_space=pltpu.VMEM),
            pl.BlockSpec(memory_space=pltpu.VMEM),
        ],
    )


def finish_kernel(g_ref, own_ref, o_ref):
    member = lax.broadcasted_iota(jnp.int32, (128, 2048), 0) == own_ref[0:1, :]
    s = jnp.where(member, 1.0, 0.0).astype(BF)
    place = lax.broadcasted_iota(jnp.int32, (64, 2048), 0) == own_ref[1:2, :]
    t = sum(mm_tn(v, s) for v in split3(g_ref[...]))
    for c in range(2):
        o_ref[c : c + 1, :] = jnp.sum(jnp.where(place, t[c * 64 : (c + 1) * 64, :], 0.0), axis=0, keepdims=True)


def finish(speeds, own):
    return call(finish_kernel, jax.ShapeDtypeStruct((2, 2048), F32), [], speeds, own)


def shards(vorticity, tile_list, float_slot, float_cell, float_frac):
    both = ("gx", "gy")
    device = lax.axis_index(both)
    exchange = functools.partial(lax.all_to_all, split_axis=0, concat_axis=0, tiled=True)
    rows = exchange(cast_block(vorticity), "gy")
    message, own = plan_floats(tile_list, float_slot, float_cell, float_frac)
    message = exchange(message.reshape(128, 1, 384), both).reshape(128, 384)
    tiles = message[:, 256].astype(jnp.int32)
    half = exchange(rows_forward(rows.reshape(64, 64, 128)), both)
    mixed = exchange(cols_step(half, device), both)
    coeffs = exchange(rows_back(mixed), "gy")
    speeds = interpolate(tiles, coeffs, message)
    speeds = exchange(speeds.reshape(128, 1, 128), both).reshape(128, 128)
    return finish(speeds, own)


def solution(mesh):
    in_specs = (
        P("gx", "gy"),
        P(("gx", "gy"), None),
        P(("gx", "gy")),
        P(None, ("gx", "gy")),
        P(None, ("gx", "gy")),
    )
    out_specs = P(None, ("gx", "gy"))
    return jax.shard_map(shards, mesh=mesh, in_specs=in_specs, out_specs=out_specs, check_vma=False)
```

```python
import functools
import math

import jax
import jax.numpy as jnp
import numpy as np
from jax import lax
from jax.experimental import pallas as pl
from jax.experimental.pallas import tpu as pltpu
from jax.sharding import PartitionSpec as P

N = 8192
KAPPA = math.pi / N
BF = jnp.bfloat16
F32 = jnp.float32
VMEM = 30 * 1024 * 1024


def _mul_const(v, c, s):
    re, im = v
    if abs(s) < 1e-12:
        if abs(c - 1.0) < 1e-12:
            return v
        if abs(c + 1.0) < 1e-12:
            return _sub((None, None), v)
    if abs(c) < 1e-12:
        return _times_i(v, s)
    if re is None:
        return (im * -s, im * c)
    if im is None:
        return (re * c, re * s)
    if abs(abs(c) - abs(s)) < 1e-12:
        q = abs(c)
        a, b = (1 if c > 0 else -1), (1 if s > 0 else -1)
        if a == b:
            return ((re - im) * (q * a), (re + im) * (q * a))
        return ((re + im) * (q * a), (im - re) * (q * a))
    return (re * c - im * s, re * s + im * c)


def _add(x, y):
    def one(p, q):
        if p is None:
            return q
        return p if q is None else p + q

    return (one(x[0], y[0]), one(x[1], y[1]))


def _sub(x, y):
    def one(p, q):
        if q is None:
            return p
        return -q if p is None else p - q

    return (one(x[0], y[0]), one(x[1], y[1]))


def _times_i(v, sign):
    re, im = v
    if sign > 0:
        return (None if im is None else -im, re)
    return (im, None if re is None else -re)


def fft_list(xs, sign):
    n = len(xs)
    if n == 1:
        return xs
    if n == 2:
        return [_add(xs[0], xs[1]), _sub(xs[0], xs[1])]
    if n == 4:
        s, d = _add(xs[0], xs[2]), _sub(xs[0], xs[2])
        t, e = _add(xs[1], xs[3]), _times_i(_sub(xs[1], xs[3]), sign)
        return [_add(s, t), _add(d, e), _sub(s, t), _sub(d, e)]
    outer = 4 if n % 4 == 0 and n > 8 else 2
    inner = n // outer
    cols = [fft_list(xs[j::outer], sign) for j in range(outer)]
    out = [None] * n
    for k0 in range(inner):
        row = []
        for j in range(outer):
            ang = sign * 2.0 * math.pi * j * k0 / n
            row.append(_mul_const(cols[j][k0], math.cos(ang), math.sin(ang)))
        for k1, v in enumerate(fft_list(row, sign)):
            out[k0 + inner * k1] = v
    return out


def split2(x):
    hi = x.astype(BF)
    return hi, (x - hi.astype(F32)).astype(BF)


def table_split(t):
    t = np.asarray(t, np.float64)
    hi = t.astype(np.float32).astype(jnp.bfloat16)
    lo = (t - hi.astype(np.float64)).astype(np.float32).astype(jnp.bfloat16)
    return hi, lo


def mm(a, b):
    return lax.dot_general(a, b, (((1,), (0,)), ((), ())), preferred_element_type=F32)


def mm_nt(a, b):
    return lax.dot_general(a, b, (((1,), (1,)), ((), ())), preferred_element_type=F32)


def mm_tn(a, b):
    return lax.dot_general(a, b, (((0,), (0,)), ((), ())), preferred_element_type=F32)


def call(kernel, out_shape, scratch, *args, specs=None):
    params = dict(
        out_shape=out_shape,
        scratch_shapes=scratch,
        compiler_params=pltpu.CompilerParams(vmem_limit_bytes=VMEM),
    )
    if specs is not None:
        params["in_specs"] = specs
    return pl.pallas_call(kernel, **params)(*args)


def cast_kernel(x_ref, o_ref):
    s = lax.broadcasted_iota(jnp.int32, (8, 8, 128), 1)

    def handed(x, rows, shift):
        error = jnp.where(rows, x.astype(BF).astype(F32) - x, 0.0)
        return x - pltpu.roll(error, shift, 1)

    for d in range(4):
        for q in range(4):
            x = x_ref[d * 64 : (d + 1) * 64, q * 128 : (q + 1) * 128].reshape(8, 8, 128)
            x = handed(x, s % 2 == 0, 1)
            x = handed(x, s % 4 == 1, 2)
            o_ref[d, q] = x.reshape(64, 128).astype(BF)


def cast_block(vorticity):
    return pl.pallas_call(
        cast_kernel,
        grid=(4,),
        in_specs=[pl.BlockSpec((256, 512), lambda i: (i, 0))],
        out_specs=pl.BlockSpec((4, 4, 64, 128), lambda i: (i, 0, 0, 0)),
        out_shape=jax.ShapeDtypeStruct((16, 4, 64, 128), BF),
    )(vorticity)


def rows_kernel(x_ref, m_ref, twr_ref, twi_ref, thi_ref, tlo_ref, alt_ref, o_ref, a_ref, yhi_ref, ylo_ref):
    def first(t, carry):
        rows = pl.ds(pl.multiple_of(t * 16, 16), 16)
        for j in range(8):
            xs = [(x_ref[8 * i + j, rows, :].astype(F32), None) for i in range(8)]
            ys = fft_list(xs, -1.0)
            for k0 in range(5):
                ang = -2.0 * math.pi * j * k0 / 64
                re, im = _mul_const(ys[k0], math.cos(ang), math.sin(ang))
                zero = jnp.zeros((16, 128), F32)
                a_ref[k0, j, 0, rows, :] = zero if re is None else re
                a_ref[k0, j, 1, rows, :] = zero if im is None else im
        return carry

    lax.fori_loop(0, 4, first, 0)

    def put(k, re, im, rows):
        cr, ci = twr_ref[k], twi_ref[k]
        yr, yi = re * cr - im * ci, re * ci + im * cr
        hr, lr = split2(yr)
        hi, li = split2(yi)
        yhi_ref[k, rows, 0:128] = hr
        yhi_ref[k, rows, 128:256] = hi
        ylo_ref[k, rows, 0:128] = lr
        ylo_ref[k, rows, 128:256] = li

    def second(t, carry):
        rows = pl.ds(pl.multiple_of(t * 16, 16), 16)
        for k0 in range(5):
            zs = fft_list([(a_ref[k0, j, 0, rows, :], a_ref[k0, j, 1, rows, :]) for j in range(8)], -1.0)
            for k1 in range(8):
                k = k0 + 8 * k1
                re, im = zs[k1]
                put(k, re, im, rows)
                if k0 in (1, 2, 3):
                    put(64 - k, re, -im, rows)
        return carry

    lax.fori_loop(0, 4, second, 0)

    def third(kap, carry):
        yhi = yhi_ref[pl.ds(2 * kap, 2)].reshape(128, 256)
        ylo = ylo_ref[pl.ds(2 * kap, 2)].reshape(128, 256)
        z = mm_nt(thi_ref[...], yhi) + mm_nt(tlo_ref[...], yhi) + mm_nt(thi_ref[...], ylo)
        zb = z.astype(BF)
        for g in range(4):
            for c in range(2):
                o_ref[4 * kap + g, 16 * c : 16 * c + 16, :] = zb[c * 64 + 16 * g : c * 64 + 16 * g + 16, :]
            o_ref[4 * kap + g, 32:40, :] = m_ref[4 * kap + g]
        return carry

    lax.fori_loop(0, 32, third, 0, unroll=4)

    nyq = mm_nt(alt_ref[...], yhi_ref[0:2].reshape(128, 256)) + mm_nt(
        alt_ref[...], ylo_ref[0:2].reshape(128, 256)
    )
    lane = lax.broadcasted_iota(jnp.int32, (16, 128), 1)
    sub = lax.broadcasted_iota(jnp.int32, (16, 128), 0)
    old = o_ref[0, 16:32, :].astype(F32)
    o_ref[0, 16:32, :] = jnp.where((lane < 64) & (sub == 0), nyq, old).astype(BF)


@functools.cache
def rows_tables():
    k = np.arange(64)[:, None, None]
    b = np.arange(128)[None, None, :]
    tw = np.exp(-2j * np.pi * k * b / N)
    w = np.exp(-2j * np.pi * np.arange(64)[:, None] * np.arange(128)[None, :] / 128)
    t = np.block([[w.real, -w.imag], [w.imag, w.real]])
    alt = np.zeros((16, 256))
    alt[0, :128] = (-1.0) ** np.arange(128)
    hi, lo = table_split(t)
    return (
        tw.real.astype(np.float32),
        tw.imag.astype(np.float32),
        hi,
        lo,
        alt.astype(np.float32).astype(jnp.bfloat16),
    )


def rows_forward(x, message):
    return call(
        rows_kernel,
        jax.ShapeDtypeStruct((128, 40, 128), BF),
        [
            pltpu.VMEM((5, 8, 2, 64, 128), F32),
            pltpu.VMEM((64, 64, 256), BF),
            pltpu.VMEM((64, 64, 256), BF),
        ],
        x,
        message,
        *rows_tables(),
    )


def fft128(load, store, a_ref, rows, sign):
    for j in range(8):
        ys = fft_list([load(8 * i + j) for i in range(16)], sign)
        for k0 in range(16):
            ang = sign * 2.0 * math.pi * j * k0 / 128
            re, im = _mul_const(ys[k0], math.cos(ang), math.sin(ang))
            a_ref[k0, j, 0, rows, :] = re
            a_ref[k0, j, 1, rows, :] = im
    for k0 in range(16):
        zs = fft_list([(a_ref[k0, j, 0, rows, :], a_ref[k0, j, 1, rows, :]) for j in range(8)], sign)
        for k1 in range(8):
            store(k0 + 16 * k1, zs[k1])


def cols_kernel(
    x_ref, twr_ref, twi_ref, tw2r_ref, tw2i_ref, fhi_ref, flo_ref, bhi_ref, blo_ref,
    wm2_ref, pm_ref, sm_ref, del_ref, wn2_ref, pn_ref, sn_ref, hm_ref,
    o_ref,
    x32_ref, a_ref, yhi_ref, ylo_ref, e_ref, ce_ref, z_ref, shi_ref, slo_ref, p_ref,
):
    def widen(t, carry):
        for u in range(8):
            for c in range(2):
                x32_ref[8 * t + u, c] = x_ref[8 * t + u, 16 * c : 16 * c + 16, :].astype(F32)
        return carry

    lax.fori_loop(0, 16, widen, 0)

    def forward(hh, carry):
        rows = pl.ds(pl.multiple_of(hh * 8, 8), 8)

        def store(k, v):
            re, im = v
            cr, ci = twr_ref[k], twi_ref[k]
            yr, yi = re * cr - im * ci, re * ci + im * cr
            x32_ref[k, 0, rows, :] = yr
            x32_ref[k, 1, rows, :] = yi

            @pl.when(hh == 0)
            def _():
                back = (128 - k) % 128
                e_ref[0, back : back + 1, :] = re[0:1, :]
                e_ref[1, back : back + 1, :] = -im[0:1, :]

        fft128(lambda d: (x32_ref[d, 0, rows, :], x32_ref[d, 1, rows, :]), store, a_ref, rows, -1.0)
        return carry

    lax.fori_loop(0, 2, forward, 0)

    def second_split(t, carry):
        for u in range(8):
            k = 8 * t + u
            rows = pl.ds(pl.multiple_of(k * 16, 16), 16)
            hr, lr = split2(x32_ref[k, 0])
            hi, li = split2(x32_ref[k, 1])
            yhi_ref[rows, 0:128] = hr
            yhi_ref[rows, 128:256] = hi
            ylo_ref[rows, 0:128] = lr
            ylo_ref[rows, 128:256] = li
        return carry

    lax.fori_loop(0, 16, second_split, 0)

    fhi, flo = fhi_ref[...], flo_ref[...]

    er, ei = e_ref[0], e_ref[1]
    cr, ci = tw2r_ref[...], tw2i_ref[...]
    e_r, e_i = er * cr - ei * ci, er * ci + ei * cr
    hr, lr = split2(e_r)
    hi, li = split2(e_i)
    ehi = jnp.concatenate([hr, hi], axis=1)
    elo = jnp.concatenate([lr, li], axis=1)
    ce = mm(ehi, fhi) + mm(elo, fhi) + mm(ehi, flo)
    ce_ref[0] = ce[:, 0:128]
    ce_ref[1] = ce[:, 128:256]

    def matmul_f(t, carry):
        rows = pl.ds(pl.multiple_of(t * 256, 256), 256)
        z_ref[rows, :] = mm(yhi_ref[rows, :], fhi) + mm(ylo_ref[rows, :], fhi) + mm(yhi_ref[rows, :], flo)
        return carry

    lax.fori_loop(0, 8, matmul_f, 0)

    wn2, pn, sn, hm = wn2_ref[...], pn_ref[...], sn_ref[...], hm_ref[...]

    def spectral(t, carry):
        for u in range(8):
            k = 8 * t + u
            rows = pl.ds(pl.multiple_of(k * 16, 16), 16)
            zr, zi = z_ref[rows, 0:128], z_ref[rows, 128:256]
            fac = 1.0 / ((wm2_ref[k] + wn2 + KAPPA * KAPPA) * (pm_ref[k] * pn))
            dd = del_ref[k] * hm
            fr = fac * zr + dd * (ce_ref[0, pl.ds(k, 1), :] - zr)
            fi = fac * zi + dd * (ce_ref[1, pl.ds(k, 1), :] - zi)
            sm = sm_ref[k]
            for f, (re, im) in enumerate(((-sm * fi, sm * fr), (sn * fi, -sn * fr))):
                hr, lr = split2(re)
                hi, li = split2(im)
                shi_ref[f, rows, 0:128] = hr
                shi_ref[f, rows, 128:256] = hi
                slo_ref[f, rows, 0:128] = lr
                slo_ref[f, rows, 128:256] = li
        return carry

    lax.fori_loop(0, 16, spectral, 0)

    bhi, blo = bhi_ref[...], blo_ref[...]

    for f in range(2):

        def matmul_b(t, carry):
            rows = pl.ds(pl.multiple_of(t * 256, 256), 256)
            hi, lo = shi_ref[f, rows, :], slo_ref[f, rows, :]
            p_ref[rows, :] = mm(hi, bhi) + mm(lo, bhi) + mm(hi, blo)
            return carry

        lax.fori_loop(0, 8, matmul_b, 0)

        def inverse(hh, carry):
            rows = pl.ds(pl.multiple_of(hh * 8, 8), 8)

            def load(k):
                at = pl.ds(pl.multiple_of(k * 16 + hh * 8, 8), 8)
                re, im = p_ref[at, 0:128], p_ref[at, 128:256]
                cr, ci = twr_ref[k], twi_ref[k]
                return (re * cr + im * ci, im * cr - re * ci)

            def store(k, v):
                x32_ref[k, 0, rows, :] = v[0]
                x32_ref[k, 1, rows, :] = v[1]

            fft128(load, store, a_ref, rows, 1.0)
            return carry

        lax.fori_loop(0, 2, inverse, 0)

        def narrow(t, carry):
            for u in range(8):
                o_ref[8 * t + u, f] = x32_ref[8 * t + u].astype(BF)
            return carry

        lax.fori_loop(0, 16, narrow, 0)


def _wave(j, length):
    signed = np.where(j < length // 2, j, j - length).astype(np.float64)
    return 2.0 * np.pi / length * signed


@functools.cache
def cols_tables():
    lane = np.arange(128)
    kk = np.arange(128)[:, None]
    tw = np.exp(-2j * np.pi * kk * (lane % 64)[None, :] / N)
    w = np.exp(-2j * np.pi * np.outer(np.arange(64), np.arange(64)) / 64)
    eye = np.eye(2)
    wr, wi = np.kron(eye, w.real), np.kron(eye, w.imag)
    forward = np.block([[wr, wi], [-wi, wr]])
    backward = np.block([[wr, -wi], [wi, wr]])
    m = kk + 128 * (lane % 64)[None, :]
    wm = _wave(m, N)
    sm = np.where(m == N // 2, 0.0, wm)
    pm = (2.0 + np.cos(wm)) / 3.0
    f0 = 1.0 / ((wm**2 + KAPPA**2) * pm * float(N) ** 2)
    f1 = 1.0 / ((wm**2 + math.pi**2 + KAPPA**2) * pm * (1.0 / 3.0) * float(N) ** 2)
    delta = (f0 - f1) / 2.0

    def three(t):
        return np.asarray(t, np.float32)[:, None, :]

    twr, twi = tw.real.astype(np.float32), tw.imag.astype(np.float32)
    return (
        (three(twr), three(twi), twr, twi, *table_split(forward), *table_split(backward)),
        (three(wm**2), three(pm), three(sm), three(delta)),
    )


def cols_step(x, device):
    first, second = cols_tables()
    h = lax.broadcasted_iota(jnp.int32, (16, 128), 0)
    p = lax.broadcasted_iota(jnp.int32, (16, 128), 1) // 64
    n = 2 * (device // 4) + p + 64 * (16 * (device % 4) + h)
    wn = (2.0 * math.pi / N) * n.astype(F32)
    pn = (2.0 + jnp.cos(wn)) / 3.0 * (float(N) ** 2)
    pn = jnp.where(n == 0, pn, pn * 0.5)
    hm = jnp.where(n == 0, 1.0, 0.0).astype(F32)
    return call(
        cols_kernel,
        jax.ShapeDtypeStruct((128, 2, 2, 16, 128), BF),
        [
            pltpu.VMEM((128, 2, 16, 128), F32),
            pltpu.VMEM((16, 8, 2, 16, 128), F32),
            pltpu.VMEM((2048, 256), BF),
            pltpu.VMEM((2048, 256), BF),
            pltpu.VMEM((2, 128, 128), F32),
            pltpu.VMEM((2, 128, 128), F32),
            pltpu.VMEM((2048, 256), F32),
            pltpu.VMEM((2, 2048, 256), BF),
            pltpu.VMEM((2, 2048, 256), BF),
            pltpu.VMEM((2048, 256), F32),
        ],
        x, *first, *second, wn * wn, pn, wn, hm,
    )


def back_kernel(x_ref, t_ref, t0r_ref, t0i_ref, omr_ref, omi_ref, alt_ref, o_ref, s_ref, f_ref):
    table = t_ref[...]

    def first(kap, carry):
        cols = []
        for f in range(2):
            re = x_ref[pl.ds(4 * kap, 4), f, 0].reshape(64, 128)
            im = x_ref[pl.ds(4 * kap, 4), f, 1].reshape(64, 128)
            cols.append(jnp.concatenate([re, im, re, im], axis=0))
        s_ref[kap] = mm(table, jnp.concatenate(cols, axis=1))
        return carry

    lax.fori_loop(0, 32, first, 0, unroll=4)

    row = x_ref[0, 0, 1].astype(F32)[0:1, :]
    lane = lax.broadcasted_iota(jnp.int32, (128, 128), 1)
    s_ref[0, 0:128, 0:128] += jnp.where(lane < 64, alt_ref[...] * row, 0.0)

    low = lax.broadcasted_iota(jnp.int32, (8, 128), 1) < 64

    def second(t, carry):
        at = pl.ds(pl.multiple_of(t * 8, 8), 8)
        ati = pl.ds(pl.multiple_of(128 + t * 8, 8), 8)
        omr, omi = omr_ref[at, :], omi_ref[at, :]
        for f in range(2):
            tr, ti = t0r_ref[at, :], t0i_ref[at, :]
            xs = []
            for kap in range(32):
                re = s_ref[kap, at, f * 128 : (f + 1) * 128]
                im = s_ref[kap, ati, f * 128 : (f + 1) * 128]
                xs.append((re * tr - im * ti, re * ti + im * tr))
                tr, ti = tr * omr - ti * omi, tr * omi + ti * omr
            ys = fft_list(xs, 1.0)
            ts = []
            for x1 in range(32):
                re, im = ys[x1]
                ang = 2.0 * math.pi * x1 / 64
                ts.append(jnp.where(low, re, re * math.cos(ang) - im * math.sin(ang)))
            for e in range(16):
                ta, tb = ts[2 * e], ts[2 * e + 1]
                even = jnp.where(low, ta, pltpu.roll(tb, 64, 1))
                odd = jnp.where(low, pltpu.roll(ta, 64, 1), tb)
                f_ref[e // 2, f, e % 2, at, :] = even + odd
                f_ref[e // 2 + 8, f, e % 2, at, :] = even - odd
        return carry

    lax.fori_loop(0, 16, second, 0)

    def narrow(j, carry):
        o_ref[j] = f_ref[j].astype(BF)
        return carry

    lax.fori_loop(0, 16, narrow, 0)


@functools.cache
def back_tables():
    x0 = np.arange(128)
    e = np.exp(2j * np.pi * np.outer(x0, np.arange(64)) / 128)
    t = np.block([[e.real, -e.imag], [e.imag, e.real]])
    hi, lo = table_split(t)
    p = np.arange(128)[None, :] // 64
    t0 = np.exp(2j * np.pi * p * x0[:, None] / N)
    om = np.exp(2j * np.pi * 2 * x0[:, None] / N) * np.ones((1, 128))
    alt = ((-1.0) ** x0)[:, None] * np.ones((1, 128))
    f = lambda v: np.ascontiguousarray(v, np.float32)
    return (np.concatenate([hi, lo], axis=1), f(t0.real), f(t0.imag), f(om.real), f(om.imag), f(alt))


def rows_back(x):
    return call(
        back_kernel,
        jax.ShapeDtypeStruct((16, 2, 2, 128, 128), BF),
        [pltpu.VMEM((32, 256, 256), F32), pltpu.VMEM((16, 2, 2, 128, 128), F32)],
        x,
        *back_tables(),
    )


def split3(x):
    hi = x.astype(BF)
    rest = x - hi.astype(F32)
    mid = rest.astype(BF)
    return hi, mid, (rest - mid.astype(F32)).astype(BF)


def plan_kernel(list_ref, slot_ref, cell_ref, frac_ref, tri_ref, msg_ref, own_ref, s_ref, r_ref, v_ref):
    slot = slot_ref[...]
    pick = lax.broadcasted_iota(jnp.int32, (64, 2048), 0) == slot
    tile = jnp.sum(jnp.where(pick, list_ref[...], 0), axis=0, keepdims=True)
    grid_row, grid_col = tile // 64, tile % 64
    owner = (grid_row // 8) * 16 + grid_col // 4
    local = ((grid_row % 8) * 4 + grid_col % 4).astype(F32)
    member = lax.broadcasted_iota(jnp.int32, (128, 2048), 0) == owner
    s_ref[...] = jnp.where(member, 1.0, 0.0).astype(BF)
    running = jnp.zeros((128, 1), F32)
    tri = tri_ref[...]
    for c in range(8):
        at = slice(c * 256, (c + 1) * 256)
        part = s_ref[:, at]
        total = mm(part, tri) + running
        rank = jnp.sum(part.astype(F32) * total, axis=0, keepdims=True) - 1.0
        running = total[:, 255:256]
        own_ref[1:2, at] = rank.astype(jnp.int32)
    own_ref[0:1, :] = owner
    rank = own_ref[1:2, :]
    place = lax.broadcasted_iota(jnp.int32, (128, 2048), 0) == rank
    r_ref[...] = jnp.where(place, 1.0, 0.0).astype(BF)
    hi0, lo0 = split2(frac_ref[0:1, :])
    hi1, lo1 = split2(frac_ref[1:2, :])
    parts = [cell_ref[0:1, :], cell_ref[1:2, :], local, hi0, lo0, hi1, lo1]
    sub = lax.broadcasted_iota(jnp.int32, (16, 2048), 0)
    values = jnp.zeros((16, 2048), F32)
    for v, part in enumerate(parts):
        values = jnp.where(sub % 8 == v, part.astype(F32), values)
    pair = owner - sub // 8

    def spread(t, carry):
        v_ref[pl.ds(pl.multiple_of(16 * t, 16), 16), :] = jnp.where(pair == 2 * t, values, 0.0).astype(BF)
        return carry

    lax.fori_loop(0, 64, spread, 0, unroll=2)
    out = mm_nt(v_ref[...], r_ref[...]).astype(BF)
    msg_ref[...] = out.reshape(128, 8, 128)


def plan_floats(tile_list, float_slot, float_cell, float_frac):
    tri = np.triu(np.ones((256, 256), np.float32)).astype(jnp.bfloat16)
    return call(
        plan_kernel,
        (
            jax.ShapeDtypeStruct((128, 8, 128), BF),
            jax.ShapeDtypeStruct((2, 2048), jnp.int32),
        ),
        [pltpu.VMEM((128, 2048), BF), pltpu.VMEM((128, 2048), BF), pltpu.VMEM((1024, 2048), BF)],
        tile_list.reshape(64, 1),
        float_slot.reshape(1, 2048),
        float_cell,
        float_frac,
        tri,
    )


def weights_of(t):
    s = 1.0 - t
    cubed = t * t * t
    return (
        s * s * s / 6.0,
        (3.0 * cubed - 6.0 * t * t + 4.0) / 6.0,
        (-3.0 * cubed + 3.0 * t * t + 3.0 * t + 1.0) / 6.0,
        cubed / 6.0,
    )


def chain(e, ws):
    zero = jnp.zeros_like(ws[0])
    out = jnp.where(e == 3.0, ws[3], zero)
    for i in (2, 1, 0):
        out = jnp.where(e == float(i), ws[i], out)
    return out


def interp_kernel(tile_ref, c_ref, msg_ref, o_ref, m_ref, w_ref, r_ref):
    low = lax.broadcasted_iota(jnp.int32, (64, 128), 1) < 64
    low8 = lax.broadcasted_iota(jnp.int32, (8, 128), 1) < 64
    for i in range(64):
        other = pltpu.roll(msg_ref[i + 64].astype(F32), 64, 1)
        m_ref[8 * i : 8 * i + 8, :] = jnp.where(low8, msg_ref[i].astype(F32), other)

    def row(v):
        return m_ref[pl.ds(v, 64, stride=8), :]

    w_ref[0] = row(0) - 1.0
    w_ref[1] = row(1) - 1.0
    for i, w in enumerate(weights_of(row(3) + row(4))):
        w_ref[2 + i] = w.astype(BF).astype(F32)
    for i, w in enumerate(weights_of(row(5) + row(6))):
        w_ref[6 + i] = w

    iota64 = lax.broadcasted_iota(jnp.int32, (64, 128), 0).astype(F32)
    iota128 = lax.broadcasted_iota(jnp.int32, (128, 128), 0).astype(F32)
    lowrow = lax.broadcasted_iota(jnp.int32, (1, 128), 1) < 64
    low128 = lax.broadcasted_iota(jnp.int32, (128, 128), 1) < 64

    def step(i, carry):
        ta, tb = tile_ref[i], tile_ref[i + 64]
        par = jnp.where(lowrow, (ta % 2).astype(F32), (tb % 2).astype(F32))
        rows = [w_ref[v, pl.ds(i, 1), :] for v in range(10)]
        blocks = []
        for half in range(2):
            for xp in range(2):
                base = rows[0] - 64.0 * half + 1000.0 * jnp.abs(par - xp)
                blocks.append(chain(iota64 - base, [jnp.broadcast_to(w, (64, 128)) for w in rows[2:6]]))
        down = jnp.concatenate(blocks, axis=0).astype(BF)
        across = chain(iota128 - rows[1], [jnp.broadcast_to(w, (128, 128)) for w in rows[6:10]])
        for f in range(2):
            inner = []
            for tile in (ta, tb):
                tr, xh = tile // 4, (tile % 4) // 2
                lhs = jnp.concatenate([c_ref[2 * tr, f, xh], c_ref[2 * tr + 1, f, xh]], axis=1)
                inner.append(mm(lhs, down))
            both = jnp.where(low128, inner[0], inner[1])
            r_ref[f, pl.ds(i, 1), :] = jnp.sum(both * across, axis=0, keepdims=True)
        return carry

    lax.fori_loop(0, 64, step, 0, unroll=4)
    u, v = r_ref[0], r_ref[1]
    o_ref[0:64, :] = jnp.where(low, u, pltpu.roll(v, 64, 1))
    o_ref[64:128, :] = jnp.where(low, pltpu.roll(u, 64, 1), v)


def interpolate(tiles, coeffs, message):
    return call(
        interp_kernel,
        jax.ShapeDtypeStruct((128, 128), F32),
        [
            pltpu.VMEM((512, 128), F32),
            pltpu.VMEM((10, 64, 128), F32),
            pltpu.VMEM((2, 64, 128), F32),
        ],
        tiles,
        coeffs,
        message,
        specs=[
            pl.BlockSpec(memory_space=pltpu.SMEM),
            pl.BlockSpec(memory_space=pltpu.VMEM),
            pl.BlockSpec(memory_space=pltpu.VMEM),
        ],
    )


def finish_kernel(g_ref, own_ref, o_ref):
    member = lax.broadcasted_iota(jnp.int32, (128, 2048), 0) == own_ref[0:1, :]
    s = jnp.where(member, 1.0, 0.0).astype(BF)
    place = lax.broadcasted_iota(jnp.int32, (64, 2048), 0) == own_ref[1:2, :]
    t = sum(mm_tn(v, s) for v in split3(g_ref[...]))
    for c in range(2):
        o_ref[c : c + 1, :] = jnp.sum(jnp.where(place, t[c * 64 : (c + 1) * 64, :], 0.0), axis=0, keepdims=True)


def finish(speeds, own):
    return call(finish_kernel, jax.ShapeDtypeStruct((2, 2048), F32), [], speeds, own)


def shards(vorticity, tile_list, float_slot, float_cell, float_frac):
    both = ("gx", "gy")
    device = lax.axis_index(both)
    exchange = functools.partial(lax.all_to_all, split_axis=0, concat_axis=0, tiled=True)
    rows = exchange(cast_block(vorticity), "gy")
    message, own = plan_floats(tile_list, float_slot, float_cell, float_frac)
    half = exchange(rows_forward(rows.reshape(64, 64, 128), message), both)
    message = half[:, 32:40, :]
    tiles = message[:, 2, 0].astype(jnp.int32)
    mixed = exchange(cols_step(half, device), both)
    coeffs = exchange(rows_back(mixed), "gy")
    speeds = interpolate(tiles, coeffs, message)
    speeds = exchange(speeds.reshape(128, 1, 128), both).reshape(128, 128)
    return finish(speeds, own)


def solution(mesh):
    in_specs = (
        P("gx", "gy"),
        P(("gx", "gy"), None),
        P(("gx", "gy")),
        P(None, ("gx", "gy")),
        P(None, ("gx", "gy")),
    )
    out_specs = P(None, ("gx", "gy"))
    return jax.shard_map(shards, mesh=mesh, in_specs=in_specs, out_specs=out_specs, check_vma=False)
```
